16 devices in a mesh: rep: 1, r: 2 (over z), s: 8 (over x, y, core).
Axes of the slice: x: 2, y: 2, z: 2, core: 2. Of those that a mesh axis runs over, the one named last changes fastest.
Arguments:
- x: bfloat16 [16, 2048, 1024], P(('rep', 'r', 's'))
- dy: bfloat16 [16, 2048, 1024], P(('rep', 'r', 's'))
- w_gate: bfloat16 [2, 1024, 3200], P(None, 's')
- w_up: bfloat16 [2, 1024, 3200], P(None, 's')
- w_down: bfloat16 [2, 3200, 1024], P(None, 's')
Outputs:
- output 1: bfloat16 [16, 2048, 1024], P(('rep', 'r', 's'))
- output 2: bfloat16 [2, 1024, 3200], P('rep', 's')
- output 3: bfloat16 [2, 1024, 3200], P('rep', 's')
- output 4: bfloat16 [2, 3200, 1024], P('rep', 's')
All inputs are finite; a program needn't handle non-finite values.
Results may differ from the reference program's by a relative error of at most 0.018.
Values are sent between devices in bfloat16 or wider.
A program may use at most 2 GiB of HBM per device.

```python
import jax
import jax.numpy as jnp
from jax import lax

SEQUENCES = 16
TOKENS = 2048
D = 1024
FF = 3200
LAYERS = 2
NAMES = ("w_gate", "w_up", "w_down")
SHAPES = {"w_gate": (LAYERS, D, FF), "w_up": (LAYERS, D, FF), "w_down": (LAYERS, FF, D)}


def bump(key, n, height):
    away = (jnp.arange(n, dtype=jnp.int32) - jax.random.randint(key, (), 0, n, jnp.int32)) % n
    return jnp.where(away < n // 8, height, 1.0)


def together(key, own, strength):
    shared = jax.random.normal(key, own.shape[1:], jnp.float32)
    return (own + strength * shared) * lax.rsqrt(1 + strength * strength)


def setup_inputs(seed: int = 0, part: int = 0) -> dict:
    kx, kdy, ka, kb, kz, kf, kh, kl, *kw = jax.random.split(jax.random.key(seed), 8 + len(NAMES))
    kx, kdy, ka, kb = (jax.random.fold_in(k, part) for k in (kx, kdy, ka, kb))
    shape = (SEQUENCES, TOKENS, D)
    much_x, much_dy = jax.random.uniform(kz, (2,), jnp.float32, 0.0, 1.0)
    layers = 2.0 ** jax.random.uniform(kl, (LAYERS, 1, 1), jnp.float32, -1.0, 1.0)
    x = together(ka, jax.random.normal(kx, shape, jnp.float32), much_x) * bump(kf, D, 4.0)
    dy = together(kb, jax.random.normal(kdy, shape, jnp.float32), much_dy)
    drawn = {"x": x.astype(jnp.bfloat16), "dy": (dy * (SEQUENCES * TOKENS) ** -0.5).astype(jnp.bfloat16)}
    for key, name in zip(kw, NAMES, strict=True):
        w = jax.random.normal(key, SHAPES[name], jnp.float32) * SHAPES[name][1] ** -0.5
        drawn[name] = (w * {"w_gate": 1.0, "w_up": bump(kh, FF, 4.0), "w_down": layers}[name]).astype(jnp.bfloat16)
    return drawn


def matmul(a, w):
    return jnp.dot(a, w, preferred_element_type=jnp.float32).astype(jnp.bfloat16)


def normed(h):
    wide = h.astype(jnp.float32)
    scale = lax.rsqrt(jnp.mean(wide**2, -1, keepdims=True) + 1e-6)
    return (wide * scale).astype(jnp.bfloat16)


def layer(h, w):
    a = normed(h)
    gate = jnp.dot(a, w["w_gate"], preferred_element_type=jnp.float32)
    up = jnp.dot(a, w["w_up"], preferred_element_type=jnp.float32)
    return h + matmul((jax.nn.silu(gate) * up).astype(jnp.bfloat16), w["w_down"])


def stack(weights, h):
    return lax.scan(lambda h, w: (layer(h, w), None), h, weights)[0]


def reference(x, dy, w_gate, w_up, w_down):
    weights = dict(zip(NAMES, (w_gate, w_up, w_down), strict=True))

    def take(so_far, sequence):
        h, by_y = sequence
        _, back = jax.vjp(stack, weights, h)
        by_weights, by_h = back(by_y)
        return jax.tree.map(lambda total, term: total + term.astype(jnp.float32), so_far, by_weights), by_h

    none_yet = {name: jnp.zeros(w.shape, jnp.float32) for name, w in weights.items()}
    by_weights, by_x = lax.scan(take, none_yet, (x, dy))
    return (by_x, *(by_weights[name].astype(jnp.bfloat16) for name in NAMES))
```

```python
import jax
import jax.numpy as jnp
from jax import lax
from jax.experimental import pallas as pl
from jax.experimental.pallas import tpu as pltpu
from jax.sharding import PartitionSpec as P

BF, F32 = jnp.bfloat16, jnp.float32
MESH = pl.DeviceIdType.MESH
T, D, F = 2048, 1024, 3200
FT, NF = 640, 5
W2 = 2 * FT
CA, CB = 3 * W2, 2 * W2


def dot(a, b, contract=((1,), (0,))):
    return lax.dot_general(a, b, (contract, ((), ())), preferred_element_type=F32)


def normed(h):
    wide = h.astype(F32)
    return (wide * lax.rsqrt(jnp.mean(wide * wide, -1, keepdims=True) + 1e-6)).astype(BF)


def rows(n, tm):
    return pl.BlockSpec((tm, n), lambda t: (t, 0))


def when_at(step, hooks):
    for at, events in hooks.items():
        @pl.when(step == at)
        def _(events=events):
            for event in events:
                event()


def norm_phase(h, a, tm=512):
    def body(h_v, a_v):
        a_v[...] = normed(h_v[...])

    pltpu.emit_pipeline(body, grid=(T // tm,), in_specs=[rows(D, tm)], out_specs=[rows(D, tm)])(h, a)


def up_phase(a, wbuf, wait_w, act, p, q, hooks, tm=512):
    nt = T // tm

    def body(a_v, act_v, p_v, q_v):
        f, t = pl.program_id(0), pl.program_id(1)
        when_at(f * nt + t, hooks)

        @pl.when(t == 0)
        def _():
            wait_w(f)

        ra = pl.ds(pl.multiple_of(t * tm, tm), tm)
        gu = dot(a_v[ra, :], wbuf[f % 2])
        g, u = gu[:, :FT], gu[:, FT:]
        s = jax.nn.sigmoid(g)
        sl = g * s
        act_v[...] = (sl * u).astype(BF)
        p_v[...] = sl
        q_v[...] = u * (s + sl * (1 - s))

    def out():
        return pl.BlockSpec((tm, FT), lambda f, t: (t, f))

    pltpu.emit_pipeline(
        body, grid=(NF, nt), in_specs=[pl.BlockSpec((T, D), lambda f, t: (0, 0))], out_specs=[out(), out(), out()]
    )(a, act, p, q)


def down_phase(act, w, h, h1, a1, hooks, tm=256):
    def body(act_v, w_v, h_v, h1_v, a1_v):
        when_at(pl.program_id(0), hooks)
        y = dot(act_v[...], w_v[...]).astype(BF)
        total = (h_v[...].astype(F32) + y.astype(F32)).astype(BF)
        h1_v[...] = total
        a1_v[...] = normed(total)

    pltpu.emit_pipeline(
        body,
        grid=(T // tm,),
        in_specs=[rows(F, tm), pl.BlockSpec((F, D), lambda t: (0, 0)), rows(D, tm)],
        out_specs=[rows(D, tm), rows(D, tm)],
    )(act, w, h, h1, a1)


def last_phase(a, wbuf, wait_w, dy, wd, act, dgu, hooks, tm=512):
    nt = T // tm

    def body(a_v, dy_v, wd_v, act_v, d_v):
        f, t = pl.program_id(0), pl.program_id(1)
        when_at(f * nt + t, hooks)

        @pl.when(t == 0)
        def _():
            wait_w(f)

        ra = pl.ds(pl.multiple_of(t * tm, tm), tm)
        gu = dot(a_v[ra, :], wbuf[f % 2])
        g, u = gu[:, :FT], gu[:, FT:]
        s = jax.nn.sigmoid(g)
        sl = g * s
        act_v[...] = (sl * u).astype(BF)
        by = dot(dy_v[ra, :], wd_v[...], ((1,), (1,))).astype(BF).astype(F32)
        d_v[:, :FT] = (by * (u * (s + sl * (1 - s)))).astype(BF)
        d_v[:, FT:] = (by * sl).astype(BF)

    def whole():
        return pl.BlockSpec((T, D), lambda f, t: (0, 0))

    pltpu.emit_pipeline(
        body,
        grid=(NF, nt),
        in_specs=[whole(), whole(), pl.BlockSpec((FT, D), lambda f, t: (f, 0))],
        out_specs=[pl.BlockSpec((tm, FT), lambda f, t: (t, f)), pl.BlockSpec((tm, W2), lambda f, t: (t, f))],
    )(a, dy, wd, act, dgu)


def hidden_phase(dy, w, p, q, dgu, f0, f1, tm=1024):
    def body(dy_v, w_v, p_v, q_v, d_v):
        ra = pl.ds(pl.multiple_of(pl.program_id(1) * tm, tm), tm)
        by = dot(dy_v[ra, :], w_v[...], ((1,), (1,))).astype(BF).astype(F32)
        d_v[:, :FT] = (by * q_v[...]).astype(BF)
        d_v[:, FT:] = (by * p_v[...]).astype(BF)

    def tile(n):
        return pl.BlockSpec((tm, n), lambda f, t: (t, f + f0))

    pltpu.emit_pipeline(
        body,
        grid=(f1 - f0, T // tm),
        in_specs=[
            pl.BlockSpec((T, D), lambda f, t: (0, 0)),
            pl.BlockSpec((FT, D), lambda f, t: (f + f0, 0)),
            tile(FT),
            tile(FT),
        ],
        out_specs=[tile(W2)],
    )(dy, w, p, q, dgu)


def by_down_phase(act, dy, o, tf=640):
    def body(a_v, d_v, o_v):
        o_v[...] = dot(a_v[...], d_v[...], ((0,), (0,))).astype(BF)

    pltpu.emit_pipeline(
        body,
        grid=(F // tf,),
        in_specs=[pl.BlockSpec((T, tf), lambda f: (0, f)), pl.BlockSpec((T, D), lambda f: (0, 0))],
        out_specs=[pl.BlockSpec((tf, D), lambda f: (f, 0))],
    )(act, dy, o)


def by_up_phase(a, dgu, o, f0, f1):
    def body(a_v, d_v, o_v):
        o_v[...] = dot(a_v[...], d_v[...], ((0,), (0,))).astype(BF)

    pltpu.emit_pipeline(
        body,
        grid=(f1 - f0,),
        in_specs=[pl.BlockSpec((T, D), lambda f: (0, 0)), pl.BlockSpec((T, W2), lambda f: (0, f + f0))],
        out_specs=[pl.BlockSpec((D, W2), lambda f: (0, f))],
    )(a, dgu, o)


def by_h_phase(dgu, w, h, dh, o, t0, t1, tm=256):
    def body(d_v, w_v, h_v, dh_v, o_v):
        by = dot(d_v[...], w_v[...], ((1,), (1,))).astype(BF).astype(F32)
        wide = h_v[...].astype(F32)
        r = lax.rsqrt(jnp.mean(wide * wide, -1, keepdims=True) + 1e-6)
        c = jnp.sum(by * wide, -1, keepdims=True) * (r * r * r) * (1.0 / D)
        back = (by * r - wide * c).astype(BF).astype(F32)
        o_v[...] = (dh_v[...].astype(F32) + back).astype(BF)

    def tile(n):
        return pl.BlockSpec((tm, n), lambda t: (t + t0 // tm, 0))

    pltpu.emit_pipeline(
        body,
        grid=((t1 - t0) // tm,),
        in_specs=[tile(2 * F), pl.BlockSpec((D, 2 * F), lambda t: (0, 0)), tile(D), tile(D)],
        out_specs=[tile(D)],
    )(dgu, w, h, dh, o)


def add_phase(steps, ins, outs):
    n = len(ins)

    def body(*refs):
        total = refs[0][...].astype(F32)
        for ref in refs[1:n]:
            total = total + ref[...].astype(F32)
        for ref in refs[n:]:
            ref[...] = total.astype(ref.dtype)

    pltpu.emit_pipeline(
        body,
        grid=(steps,),
        in_specs=[pl.BlockSpec(shape, at) for _, shape, at in ins],
        out_specs=[pl.BlockSpec(shape, at) for _, shape, at in outs],
    )(*(ref for ref, _, _ in ins), *(ref for ref, _, _ in outs))


UNITS = ((400, D), (128, CA), (128, CB), (400, D), (128, CA), (128, CB))
NAG = 14


def unit_shapes(r, c):
    h = c // 2
    return [
        ((8 * r, c), BF),
        ((4 * r, c), BF),
        ((4 * r, h), BF),
        ((4 * r, h), BF),
        ((2 * r, h), BF),
        ((2 * r, h), BF),
        ((r, c), F32),
        ((r, c), BF),
        ((r, c), BF),
    ]


def kernel(x, dy, wgu0, wgu1, wd0, wd1, *rest):
    dx, outs = rest[0], rest[1:7]
    WGU0, WGU1, WD0, WD1, a0, h1, a1, act0, act1, p, q, dgu0, dgu1, dh1 = rest[7:21]
    bufs = [rest[21 + 9 * u : 30 + 9 * u] for u in range(6)]
    wbuf, wsem, ag_send, ag_recv, ag_loc, rs_send, rs_recv = rest[75:]

    rep, z, me = lax.axis_index("rep"), lax.axis_index("r"), lax.axis_index("s")
    mx, my, mc = me // 4, (me // 2) % 2, me % 2
    sx, sy, sc = me + 4 * (1 - 2 * mx), me + 2 * (1 - 2 * my), me + (1 - 2 * mc)
    to_x, to_y, to_c, to_z = (rep, z, sx), (rep, z, sy), (rep, z, sc), (rep, 1 - z, me)
    sf, sg = sx + z * (sy - sx), sy + z * (sx - sy)
    sd = sx + sy - me
    to_f, to_g = (rep, z, sf), (rep, z, sg)

    barrier = pltpu.get_barrier_semaphore()
    for there in (to_x, to_y, to_c, to_z):
        pl.semaphore_signal(barrier, inc=1, device_id=there, device_id_type=MESH)
    pl.semaphore_wait(barrier, 4)

    def piece(u, s):
        if u < 5 or u >= 9:
            whole, own, f = (WGU0, wgu0, u) if u < 5 else (WGU1, wgu1, u - 9)
            cols = pl.ds(f * W2, W2)
            return whole.at[pl.ds(pl.multiple_of(s * 128, 128), 128), cols], own.at[:, cols]
        whole, own = (WD0, wd0) if u < 7 else (WD1, wd1)
        cols = pl.ds((u - 5) % 2 * 512, 512)
        return whole.at[pl.ds(pl.multiple_of(s * 400, 400), 400), cols], own.at[:, cols]

    def remote(src, dst, send, recv, there):
        return pltpu.make_async_remote_copy(
            src_ref=src, dst_ref=dst, send_sem=send, recv_sem=recv, device_id=there, device_id_type=MESH
        )

    def fetch(u, k, s, own, there):
        dst, mine = piece(u, s)
        return remote(mine if own else dst, dst, ag_send.at[u, k], ag_recv.at[u, k], there)

    def fetches(u, *ks):
        plan = (
            (me, True, to_f),
            (me, True, to_c),
            (sf, False, to_z),
            (sf, False, to_g),
            (sf, False, to_c),
            (sg, False, to_c),
            (sd, False, to_c),
        )
        return [fetch(u, k, *plan[k]) for k in ks]

    def arrival(u, k, s):
        dst, _ = piece(u, s)
        return remote(dst, dst, ag_send.at[u, k], ag_recv.at[u, k], to_c)

    def local(u):
        dst, mine = piece(u, me)
        return pltpu.make_async_copy(mine, dst, ag_loc.at[u])

    def start(u):
        def event():
            local(u).start()
            for copy in fetches(u, 0, 1):
                copy.start()
        return event

    def forward(u):
        def event():
            arrival(u, 0, sf).wait_recv()
            for copy in fetches(u, 2, 3, 4):
                copy.start()
        return event

    def across(u):
        def event():
            arrival(u, 2, sg).wait_recv()
            arrival(u, 3, sd).wait_recv()
            for copy in fetches(u, 5, 6):
                copy.start()
        return event

    def here(u):
        def event():
            local(u).wait()
            other = 1 - 2 * mc
            for k, s in ((1, me), (4, sf), (5, sg), (6, sd)):
                arrival(u, k, s + other).wait_recv()
            for copy in fetches(u, *range(7)):
                copy.wait_send()
        return event

    def load(whole, f):
        return pltpu.make_async_copy(whole.at[:, pl.ds(pl.multiple_of(f * W2, W2), W2)], wbuf.at[f % 2], wsem.at[f % 2])

    def start_load(whole, f):
        return lambda: load(whole, f).start()

    def remote_rs(u, k, src, dst, there):
        return remote(src, dst, rs_send.at[u, k], rs_recv.at[u, k], there)

    def cut(ref, r, i, n=1):
        return ref.at[pl.ds(pl.multiple_of(i * r, r), n * r), :]

    def rs_copies(u, stage):
        r = UNITS[u][0]
        G, RD, SB, R1, SC, R2, VF, SV, RZ = bufs[u]
        if stage == 0:
            return [remote_rs(u, j, cut(G, r, 2 * j + 1 - mc), cut(RD, r, j), to_c) for j in range(4)]
        if stage == 1:
            return [
                remote_rs(u, 4, cut(SB, r, 0, 2), cut(R1, r, 0, 2), to_x),
                remote_rs(u, 5, cut(SB, r, 2, 2), cut(R1, r, 2, 2), to_y),
            ]
        if stage == 2:
            return [
                remote_rs(u, 6, cut(SC, r, 0), cut(R2, r, 0), to_y),
                remote_rs(u, 7, cut(SC, r, 1), cut(R2, r, 1), to_x),
            ]
        return [remote_rs(u, 8, SV, RZ, to_z)]

    def rs(u, stage):
        r, c = UNITS[u]
        h = c // 2
        G, RD, SB, R1, SC, R2, VF, SV, RZ = bufs[u]
        if stage > 0:
            for copy in rs_copies(u, stage - 1):
                copy.wait()
        half = (r, h)
        own = 2 * mx + my
        if stage == 1:
            def chip(i):
                cx = (1 - mx) + (i // 2) * (1 - i % 2) * (2 * mx - 1)
                cy = my + ((i + 3) // 4) * (1 - 2 * my)
                return 2 * cx + cy
            add_phase(
                4,
                [(G, half, lambda i: (2 * chip(i) + mc, i // 2)), (RD, half, lambda i: (chip(i), i // 2))],
                [(SB, half, lambda i: (i, 0))],
            )
        if stage == 2:
            def chip(i):
                return 2 * (mx + i * (1 - 2 * mx)) + my + (1 - i) * (1 - 2 * my)
            add_phase(
                2,
                [
                    (G, half, lambda i: (2 * chip(i) + mc, i)),
                    (RD, half, lambda i: (chip(i), i)),
                    (R1, half, lambda i: (1 + 2 * i, 0)),
                ],
                [(SC, half, lambda i: (i, 0))],
            )
        if stage == 3:
            add_phase(
                2,
                [
                    (G, half, lambda i: (2 * own + mc, i)),
                    (RD, half, lambda i: (own, i)),
                    (R1, half, lambda i: (2 * i, 0)),
                    (R2, half, lambda i: (i, 0)),
                ],
                [(VF, half, lambda i: (0, i)), (SV, half, lambda i: (0, i))],
            )
        if stage == 4:
            add_phase(
                2,
                [(VF, half, lambda i: (0, i)), (RZ, half, lambda i: (0, i))],
                [(outs[u], half, lambda i: (0, i))],
            )
            return
        for copy in rs_copies(u, stage):
            copy.start()

    for u in range(3):
        start(u)()
    norm_phase(x, a0)
    for event in (forward(0), start(3), across(0), forward(1), start(4), here(0), start_load(WGU0, 0)):
        event()
    hooks = {}
    for f in range(5):
        events = hooks.setdefault(4 * f, [])
        events.append(forward(f + 2))
        events.append(start(f + 5))
        hooks[4 * f + 1] = [across(f + 1)]
        hooks[4 * f + 2] = [here(f + 1)]
        if f < 4:
            hooks[4 * f + 2].append(start_load(WGU0, f + 1))
    up_phase(a0, wbuf, lambda f: load(WGU0, f).wait(), act0, p, q, hooks)
    for event in (across(6), forward(7), start(10), here(6)):
        event()
    down_phase(
        act0,
        WD0,
        x,
        h1,
        a1,
        {2: [across(7), forward(8), start(11)], 4: [here(7), across(8), forward(9), start(12)], 6: [here(8), across(9), forward(10), start(13)]},
    )
    for event in (here(9), start_load(WGU1, 0)):
        event()
    hooks = {}
    for f in range(4):
        hooks[4 * f] = [across(f + 10)] + ([forward(f + 11)] if f < 3 else [])
        hooks[4 * f + 2] = [here(f + 10), start_load(WGU1, f + 1)]
    last_phase(a1, wbuf, lambda f: load(WGU1, f).wait(), dy, WD1, act1, dgu1, hooks)

    G = [b[0] for b in bufs]
    by_down_phase(act1, dy, G[0])
    rs(0, 0)
    by_up_phase(a1, dgu1, G[1], 0, 3)
    rs(0, 1)
    rs(1, 0)
    by_up_phase(a1, dgu1, G[2], 3, 5)
    rs(0, 2)
    rs(1, 1)
    rs(2, 0)
    by_h_phase(dgu1, WGU1, h1, dy, dh1, 0, T // 2)
    rs(0, 3)
    rs(1, 2)
    rs(2, 1)
    by_h_phase(dgu1, WGU1, h1, dy, dh1, T // 2, T)
    rs(1, 3)
    by_down_phase(act0, dh1, G[3])
    rs(3, 0)
    rs(2, 2)
    rs(0, 4)
    hidden_phase(dh1, WD0, p, q, dgu0, 0, 3)
    rs(3, 1)
    rs(2, 3)
    rs(1, 4)
    by_up_phase(a0, dgu0, G[4], 0, 3)
    rs(4, 0)
    rs(3, 2)
    hidden_phase(dh1, WD0, p, q, dgu0, 3, 5)
    rs(4, 1)
    rs(3, 3)
    rs(2, 4)
    by_up_phase(a0, dgu0, G[5], 3, 5)
    rs(5, 0)
    by_h_phase(dgu0, WGU0, x, dh1, dx, 0, T // 4)
    rs(5, 1)
    rs(4, 2)
    by_h_phase(dgu0, WGU0, x, dh1, dx, T // 4, T)
    rs(3, 4)
    rs(4, 3)
    rs(5, 2)
    rs(5, 3)
    rs(4, 4)
    rs(5, 4)


def solution(mesh):
    def step(x, dy, w_gate, w_up, w_down):
        def tiles(g, u):
            both = jnp.stack([g.reshape(128, NF, FT), u.reshape(128, NF, FT)], 2)
            return both.reshape(128, 2 * F)

        shapes = [((T, D), BF)]
        shapes += [(s, BF) for s in UNITS]
        shapes += [((D, 2 * F), BF)] * 2 + [((F, D), BF)] * 2 + [((T, D), BF)] * 3
        shapes += [((T, F), BF)] * 2 + [((T, F), F32)] * 2 + [((T, 2 * F), BF)] * 2 + [((T, D), BF)]
        for unit in UNITS:
            shapes += unit_shapes(*unit)
        anywhere = pl.BlockSpec(memory_space=pl.ANY)
        flops = 17 * 2 * T * D * F
        res = pl.pallas_call(
            kernel,
            out_shape=[jax.ShapeDtypeStruct(s, t) for s, t in shapes],
            in_specs=[anywhere] * 6,
            out_specs=[anywhere] * len(shapes),
            scratch_shapes=[
                pltpu.VMEM((2, D, W2), BF),
                pltpu.SemaphoreType.DMA((2,)),
                pltpu.SemaphoreType.DMA((NAG, 7)),
                pltpu.SemaphoreType.DMA((NAG, 7)),
                pltpu.SemaphoreType.DMA((NAG,)),
                pltpu.SemaphoreType.DMA((6, 9)),
                pltpu.SemaphoreType.DMA((6, 9)),
            ],
            compiler_params=pltpu.CompilerParams(
                collective_id=0, has_side_effects=True, vmem_limit_bytes=62 * 2**20
            ),
            cost_estimate=pl.CostEstimate(flops=flops, bytes_accessed=2**30, transcendentals=0),
            name="step",
        )(x[0], dy[0], tiles(w_gate[0], w_up[0]), tiles(w_gate[1], w_up[1]), w_down[0], w_down[1])
        dx, gd1, ga1, gb1, gd0, ga0, gb0 = res[:7]

        def untiled(a, b, i):
            return jnp.concatenate([v.reshape(128, -1, 2, FT)[:, :, i].reshape(128, -1) for v in (a, b)], -1)

        gates, ups = (jnp.stack([untiled(ga0, gb0, i), untiled(ga1, gb1, i)]) for i in range(2))
        return dx[None], gates, ups, jnp.stack([gd0, gd1])

    states, cut = P(("rep", "r", "s"), None, None), P(None, "s", None)
    return jax.shard_map(
        step,
        mesh=mesh,
        in_specs=(states, states) + (cut,) * 3,
        out_specs=(states,) + (P("rep", "s", None),) * 3,
        check_vma=False,
    )
```

```python
import jax
import jax.numpy as jnp
from jax import lax
from jax.experimental import pallas as pl
from jax.experimental.pallas import tpu as pltpu
from jax.sharding import PartitionSpec as P

BF, F32 = jnp.bfloat16, jnp.float32
MESH = pl.DeviceIdType.MESH
T, D, F = 2048, 1024, 3200
FT, NF = 640, 5
W2 = 2 * FT
CA, CB = 3 * W2, 2 * W2


NT, TN = ((1,), (1,)), ((0,), (0,))


def dot(a, b, contract=((1,), (0,))):
    return lax.dot_general(a, b, (contract, ((), ())), preferred_element_type=F32)


def normed(h):
    wide = h.astype(F32)
    return (wide * lax.rsqrt(jnp.mean(wide * wide, -1, keepdims=True) + 1e-6)).astype(BF)


def rows(n, tm):
    return pl.BlockSpec((tm, n), lambda t: (t, 0))


def origin(*_):
    return 0, 0


def when_at(step, hooks):
    for at, events in hooks.items():
        @pl.when(step == at)
        def _(events=events):
            for event in events:
                event()


def norm_phase(h, a, tm=256):
    def body(h_v, a_v):
        a_v[...] = normed(h_v[...])

    pltpu.emit_pipeline(body, grid=(T // tm,), in_specs=[rows(D, tm)], out_specs=[rows(D, tm)])(h, a)


def run(body, grid, ins, outs, sides=()):
    ins, outs = list(ins), list(outs)
    m, n = len(ins), len(outs)

    def at(steps, index):
        def block(*g):
            flat = g[0] if len(g) == 1 else g[0] * grid[1] + g[1]
            return index(jnp.minimum(flat, steps - 1))
        return block

    for steps, more, results in sides:
        ins += [(ref, shape, at(steps, index)) for ref, shape, index in more]
    for steps, more, results in sides:
        outs += [(ref, shape, at(steps, index)) for ref, shape, index in results]

    def whole(*refs):
        mains, side_ins = refs[:m], refs[m : len(ins)]
        results, side_outs = refs[len(ins) : len(ins) + n], refs[len(ins) + n :]
        body(*mains, *results)
        for _, more, sums in sides:
            total = side_ins[0][...].astype(F32)
            for ref in side_ins[1 : len(more)]:
                total = total + ref[...].astype(F32)
            for ref in side_outs[: len(sums)]:
                ref[...] = total.astype(ref.dtype)
            side_ins, side_outs = side_ins[len(more) :], side_outs[len(sums) :]

    pltpu.emit_pipeline(
        whole,
        grid=grid,
        in_specs=[pl.BlockSpec(shape, index) for _, shape, index in ins],
        out_specs=[pl.BlockSpec(shape, index) for _, shape, index in outs],
    )(*(ref for ref, _, _ in ins), *(ref for ref, _, _ in outs))


def add_phase(steps, ins, outs):
    run(lambda *refs: None, (steps,), [], [], [(steps, ins, outs)])


def join_phase(g, u, whole, me):
    def body(g_v, u_v, o_v):
        o_v[:, :FT] = g_v[...]
        o_v[:, FT:] = u_v[...]

    run(
        body,
        (NF,),
        [(g, (RU, FT), lambda f: (0, f)), (u, (RU, FT), lambda f: (0, f))],
        [(whole, (RU, W2), lambda f: (me, f))],
    )


def copy_phase(w, whole, me):
    def body(w_v, o_v):
        o_v[...] = w_v[...]

    run(body, (2,), [(w, (RD_, D // 2), lambda i: (0, i))], [(whole, (RD_, D // 2), lambda i: (me, i))])


def gated(gu):
    g, u = gu[:, :FT], gu[:, FT:]
    s = jax.nn.sigmoid(g)
    sl = g * s
    return sl, u * (s + sl * (1 - s)), sl * u


def up_phase(a, wbuf, wait_w, act, p, q, hooks, tm=1024, sub=512):
    nt, ns = T // tm, tm // sub

    def body(a_v, act_v, p_v, q_v):
        f, t = pl.program_id(0), pl.program_id(1)

        @pl.loop(0, ns)
        def _(i):
            piece = t * ns + i
            when_at(f * nt * ns + piece, hooks)

            @pl.when(piece == 0)
            def _():
                wait_w(f)

            ra, r = (pl.ds(pl.multiple_of(j * sub, sub), sub) for j in (piece, i))
            p_v[r, :], q_v[r, :], hidden = gated(dot(a_v[ra, :], wbuf[f % 2]))
            act_v[r, :] = hidden.astype(BF)

    def tile(ref):
        return ref, (tm, FT), lambda f, t: (t, f)

    run(body, (NF, nt), [(a, (T, D), origin)], [tile(act), tile(p), tile(q)])


def down_phase(act, w, h, h1, a1, hooks, tm=256):
    def body(act_v, w_v, h_v, h1_v, a1_v):
        when_at(pl.program_id(0), hooks)
        y = dot(act_v[...], w_v[...]).astype(BF)
        total = (h_v[...].astype(F32) + y.astype(F32)).astype(BF)
        h1_v[...] = total
        a1_v[...] = normed(total)

    def tile(ref, n=D):
        return ref, (tm, n), lambda t: (t, 0)

    run(body, (T // tm,), [tile(act, F), (w, (F, D), origin), tile(h)], [tile(h1), tile(a1)])


def last_phase(a, wbuf, wait_w, dy, wd, dgu, o, acc, hooks, tm=1024, sub=512):
    nt, ns = T // tm, tm // sub

    def body(a_v, dy_v, wd_v, d_v, o_v):
        f, t = pl.program_id(0), pl.program_id(1)

        @pl.loop(0, ns)
        def _(i):
            piece = t * ns + i
            when_at(f * nt * ns + piece, hooks)

            @pl.when(piece == 0)
            def _():
                wait_w(f)

            ra, r = (pl.ds(pl.multiple_of(j * sub, sub), sub) for j in (piece, i))
            p, q, hidden = gated(dot(a_v[ra, :], wbuf[f % 2]))
            by = dot(dy_v[ra, :], wd_v[...], NT).astype(BF).astype(F32)
            d_v[r, :FT] = (by * q).astype(BF)
            d_v[r, FT:] = (by * p).astype(BF)
            term = dot(hidden.astype(BF), dy_v[ra, :], TN)

            @pl.when(piece == 0)
            def _():
                acc[:FT, :] = term

            @pl.when(piece > 0)
            def _():
                acc[:FT, :] += term

        @pl.when(t == nt - 1)
        def _():
            o_v[...] = acc[:FT, :].astype(BF)

    run(
        body,
        (NF, nt),
        [(a, (T, D), origin), (dy, (T, D), origin), (wd, (FT, D), lambda f, t: (f, 0))],
        [(dgu, (tm, W2), lambda f, t: (t, f)), (o, (FT, D), lambda f, t: (f, 0))],
    )


def hidden_phase(dy, w, act, p, q, dgu, o, acc, f0, f1, sides=(), tm=1024):
    nt = T // tm

    def body(dy_v, w_v, act_v, p_v, q_v, d_v, o_v):
        t = pl.program_id(1)
        ra = pl.ds(pl.multiple_of(t * tm, tm), tm)
        by = dot(dy_v[ra, :], w_v[...], NT).astype(BF).astype(F32)
        d_v[:, :FT] = (by * q_v[...]).astype(BF)
        d_v[:, FT:] = (by * p_v[...]).astype(BF)
        term = dot(act_v[...], dy_v[ra, :], TN)

        @pl.when(t == 0)
        def _():
            acc[:FT, :] = term

        @pl.when(t == nt - 1)
        def _():
            o_v[...] = (acc[:FT, :] + term).astype(BF)

    def tile(ref, n):
        return ref, (tm, n), lambda f, t: (t, f + f0)

    def row(ref):
        return ref, (FT, D), lambda f, t: (f + f0, 0)

    run(
        body,
        (f1 - f0, nt),
        [(dy, (T, D), origin), row(w), tile(act, FT), tile(p, FT), tile(q, FT)],
        [tile(dgu, W2), row(o)],
        sides,
    )


def by_up_phase(a, dgu, o, f0, f1, sides=(), hooks={}, sub=512):
    def body(a_v, d_v, o_v):
        when_at(pl.program_id(0), hooks)

        @pl.loop(0, D // sub)
        def _(i):
            r = pl.ds(pl.multiple_of(i * sub, sub), sub)
            o_v[r, :] = dot(a_v[:, r], d_v[...], TN).astype(BF)

    run(
        body,
        (f1 - f0,),
        [(a, (T, D), origin), (dgu, (T, W2), lambda f: (0, f + f0))],
        [(o, (D, W2), lambda f: (0, f))],
        sides,
    )


def by_h_phase(dgu, w, acc, k0, k1, sides=(), hooks={}, sub=1024):
    def body(d_v, w_v):
        when_at(pl.program_id(0), hooks)
        if k0 == 0:
            @pl.when(pl.program_id(0) == 0)
            def _():
                acc[...] = jnp.zeros_like(acc)

        @pl.loop(0, T // sub)
        def _(i):
            r = pl.ds(pl.multiple_of(i * sub, sub), sub)
            acc[r, :] += dot(d_v[r, :], w_v[...], NT)

    run(
        body,
        (k1 - k0,),
        [(dgu, (T, W2), lambda k: (0, k + k0)), (w, (D, W2), lambda k: (0, k + k0))],
        [],
        sides,
    )


def by_h_end(acc, h, dh, o, tm=256):
    def body(h_v, dh_v, o_v):
        by = acc[pl.ds(pl.multiple_of(pl.program_id(0) * tm, tm), tm), :].astype(BF).astype(F32)
        wide = h_v[...].astype(F32)
        r = lax.rsqrt(jnp.mean(wide * wide, -1, keepdims=True) + 1e-6)
        c = jnp.sum(by * wide, -1, keepdims=True) * (r * r * r) * (1.0 / D)
        back = (by * r - wide * c).astype(BF).astype(F32)
        o_v[...] = (dh_v[...].astype(F32) + back).astype(BF)

    def tile(ref):
        return ref, (tm, D), lambda t: (t, 0)

    run(body, (T // tm,), [tile(h), tile(dh)], [tile(o)])


RU, RD_ = D // 8, F // 8
D1, A1, B1, D0, A0, B0 = range(6)
CORE, NEAR, FAR, GROUP = range(4)
UNITS = 2 * ((RD_, D), (RU, CA), (RU, CB))
NAG = 14


def unit_shapes(r, c):
    h = c // 2
    return [
        ((8 * r, c), BF),
        ((4 * r, c), BF),
        ((4 * r, h), BF),
        ((4 * r, h), BF),
        ((2 * r, h), BF),
        ((2 * r, h), BF),
        ((r, c), F32),
        ((r, c), BF),
        ((r, c), BF),
    ]


def kernel(x, dy, w_gate, w_up, w_down, dx, *rest):
    x, dy = x.at[0], dy.at[0]
    WGU0, WGU1, WD0, WD1, a0, h1, a1, act0, p, q, dgu0, dgu1, dh1 = rest[:13]
    bufs = [rest[13 + 9 * u :][:9] for u in range(len(UNITS))]
    wbuf, acc, wsem, ag_send, ag_recv, rs_send, rs_recv = rest[13 + 9 * len(UNITS) :]

    rep, z, me = lax.axis_index("rep"), lax.axis_index("r"), lax.axis_index("s")
    mx, my, mc = me // 4, (me // 2) % 2, me % 2
    sx, sy, sc = me + 4 * (1 - 2 * mx), me + 2 * (1 - 2 * my), me + (1 - 2 * mc)
    to_x, to_y, to_c, to_z = (rep, z, sx), (rep, z, sy), (rep, z, sc), (rep, 1 - z, me)
    sf, sg = sx + z * (sy - sx), sy + z * (sx - sy)
    sd = sx + sy - me
    to_f, to_g = (rep, z, sf), (rep, z, sg)

    barrier = pltpu.get_barrier_semaphore()
    for there in (to_x, to_y, to_c, to_z):
        pl.semaphore_signal(barrier, inc=1, device_id=there, device_id_type=MESH)
    pl.semaphore_wait(barrier, 4)

    def piece(u, s):
        if u < 5 or u >= 9:
            whole, f = (WGU0, u) if u < 5 else (WGU1, u - 9)
            return whole.at[pl.ds(pl.multiple_of(s * RU, RU), RU), pl.ds(f * W2, W2)]
        whole = WD0 if u < 7 else WD1
        return whole.at[pl.ds(pl.multiple_of(s * RD_, RD_), RD_), pl.ds((u - 5) % 2 * 512, 512)]

    def remote(src, dst, send, recv, there):
        return pltpu.make_async_remote_copy(
            src_ref=src, dst_ref=dst, send_sem=send, recv_sem=recv, device_id=there, device_id_type=MESH
        )

    def fetches(u, *ks):
        plan = ((me, to_f), (me, to_c), (sf, to_z), (sf, to_g), (sf, to_c), (sg, to_c), (sd, to_c))
        return [
            remote(piece(u, plan[k][0]), piece(u, plan[k][0]), ag_send.at[u, k], ag_recv.at[u, k], plan[k][1]) for k in ks
        ]

    def arrival(u, k, s):
        return remote(piece(u, s), piece(u, s), ag_send.at[u, k], ag_recv.at[u, k], to_c)

    def start(u):
        def event():
            for copy in fetches(u, 0, 1):
                copy.start()
        return event

    def forward(u):
        def event():
            arrival(u, 0, sf).wait_recv()
            for copy in fetches(u, 2, 3, 4):
                copy.start()
        return event

    def across(u):
        def event():
            arrival(u, 2, sg).wait_recv()
            arrival(u, 3, sd).wait_recv()
            for copy in fetches(u, 5, 6):
                copy.start()
        return event

    def here(u):
        def event():
            other = 1 - 2 * mc
            for k, s in ((1, me), (4, sf), (5, sg), (6, sd)):
                arrival(u, k, s + other).wait_recv()
            for copy in fetches(u, *range(7)):
                copy.wait_send()
        return event

    def load(whole, f):
        return pltpu.make_async_copy(whole.at[:, pl.ds(pl.multiple_of(f * W2, W2), W2)], wbuf.at[f % 2], wsem.at[f % 2])

    def start_load(whole, f):
        return lambda: load(whole, f).start()

    def remote_rs(u, k, src, dst, there):
        return remote(src, dst, rs_send.at[u, k], rs_recv.at[u, k], there)

    def cut(ref, r, i, n=1):
        return ref.at[pl.ds(pl.multiple_of(i * r, r), n * r), :]

    def rs_copies(u, stage):
        r = UNITS[u][0]
        G, RD, SB, R1, SC, R2, VF, SV, RZ = bufs[u]
        if stage == 0:
            return [remote_rs(u, j, cut(G, r, 2 * j + 1 - mc), cut(RD, r, j), to_c) for j in range(4)]
        if stage == 1:
            return [
                remote_rs(u, 4, cut(SB, r, 0, 2), cut(R1, r, 0, 2), to_x),
                remote_rs(u, 5, cut(SB, r, 2, 2), cut(R1, r, 2, 2), to_y),
            ]
        if stage == 2:
            return [
                remote_rs(u, 6, cut(SC, r, 0), cut(R2, r, 0), to_y),
                remote_rs(u, 7, cut(SC, r, 1), cut(R2, r, 1), to_x),
            ]
        return [remote_rs(u, 8, SV, RZ, to_z)]

    def sums(u, stage):
        r, c = UNITS[u]
        half = (r, c // 2)
        G, RD, SB, R1, SC, R2, VF, SV, RZ = bufs[u]
        own = 2 * mx + my
        if stage == 1:
            def side(axis):
                def chip(i):
                    cx = (1 - mx) + axis * (1 - i) * (2 * mx - 1)
                    cy = my + (1 - (1 - axis) * (1 - i)) * (1 - 2 * my)
                    return 2 * cx + cy
                return (
                    2,
                    [(G, half, lambda i: (2 * chip(i) + mc, axis)), (RD, half, lambda i: (chip(i), axis))],
                    [(SB, half, lambda i: (i + 2 * axis, 0))],
                )
            return [side(0), side(1)]
        if stage == 2:
            def chip(i):
                return 2 * (mx + i * (1 - 2 * mx)) + my + (1 - i) * (1 - 2 * my)
            return [(
                2,
                [
                    (G, half, lambda i: (2 * chip(i) + mc, i)),
                    (RD, half, lambda i: (chip(i), i)),
                    (R1, half, lambda i: (1 + 2 * i, 0)),
                ],
                [(SC, half, lambda i: (i, 0))],
            )]
        return [(
            2,
            [
                (G, half, lambda i: (2 * own + mc, i)),
                (RD, half, lambda i: (own, i)),
                (R1, half, lambda i: (2 * i, 0)),
                (R2, half, lambda i: (i, 0)),
            ],
            [(VF, half, lambda i: (0, i)), (SV, half, lambda i: (0, i))],
        )]

    def send(u, stage):
        for copy in rs_copies(u, stage):
            copy.start()

    def wait(u, stage):
        for copy in rs_copies(u, stage):
            copy.wait()

    def rs(u, stage):
        wait(u, stage - 1)
        run(lambda *refs: None, (2,), [], [], sums(u, stage))
        send(u, stage)

    join_phase(w_gate.at[0], w_up.at[0], WGU0, me)
    for u in range(3):
        start(u)()
    norm_phase(x, a0)
    forward(0)()
    start(3)()
    copy_phase(w_down.at[0], WD0, me)
    copy_phase(w_down.at[1], WD1, me)
    forward(1)()
    start(4)()
    join_phase(w_gate.at[1], w_up.at[1], WGU1, me)
    for event in (across(0), here(0), start_load(WGU0, 0)):
        event()
    hooks = {}
    for f in range(5):
        events = hooks.setdefault(4 * f, [])
        events.append(forward(f + 2))
        events.append(start(f + 5))
        hooks[4 * f + 1] = [across(f + 1)]
        hooks[4 * f + 2] = [here(f + 1)]
        if f < 4:
            hooks[4 * f + 2].append(start_load(WGU0, f + 1))
    up_phase(a0, wbuf, lambda f: load(WGU0, f).wait(), act0, p, q, hooks)
    for event in (across(6), forward(7), start(10), here(6)):
        event()
    down_phase(
        act0,
        WD0,
        x,
        h1,
        a1,
        {2: [across(7), forward(8), start(11)], 4: [here(7), across(8), forward(9), start(12)], 6: [here(8), across(9), forward(10), start(13)]},
    )
    for event in (here(9), start_load(WGU1, 0)):
        event()
    hooks = {}
    for f in range(4):
        hooks[4 * f] = [across(f + 10)] + ([forward(f + 11)] if f < 3 else [])
        hooks[4 * f + 2] = [here(f + 10), start_load(WGU1, f + 1)]
    G = [b[0] for b in bufs]
    last_phase(a1, wbuf, lambda f: load(WGU1, f).wait(), dy, WD1, dgu1, G[0], acc, hooks)

    def at_once(u, stage):
        return lambda: rs(u, stage)

    send(D1, CORE)
    by_up_phase(a1, dgu1, G[A1], 0, 3)
    send(A1, CORE)
    wait(D1, CORE)
    by_up_phase(a1, dgu1, G[B1], 3, 5, sums(D1, NEAR))
    send(D1, NEAR)
    send(B1, CORE)
    wait(A1, CORE)
    by_h_phase(dgu1, WGU1, acc, 0, 3, sums(A1, NEAR))
    send(A1, NEAR)
    wait(B1, CORE)
    wait(D1, NEAR)
    by_h_phase(dgu1, WGU1, acc, 3, 5, sums(B1, NEAR) + sums(D1, FAR))
    send(D1, FAR)
    send(B1, NEAR)
    by_h_end(acc, h1, dy, dh1)
    wait(A1, NEAR)
    hidden_phase(dh1, WD0, act0, p, q, dgu0, G[D0], acc, 0, 3, sums(A1, FAR))
    send(A1, FAR)
    wait(D1, FAR)
    wait(B1, NEAR)
    hidden_phase(dh1, WD0, act0, p, q, dgu0, G[D0], acc, 3, 5, sums(D1, GROUP) + sums(B1, FAR))
    send(D0, CORE)
    send(B1, FAR)
    send(D1, GROUP)
    wait(A1, FAR)
    by_up_phase(a0, dgu0, G[A0], 0, 3, sums(A1, GROUP), {1: [at_once(D0, NEAR)]})
    send(A0, CORE)
    send(A1, GROUP)
    wait(B1, FAR)
    by_up_phase(a0, dgu0, G[B0], 3, 5, sums(B1, GROUP), {1: [at_once(D0, FAR), at_once(A0, NEAR)]})
    send(B0, CORE)
    send(B1, GROUP)
    late = {1: [at_once(D0, GROUP)], 2: [at_once(A0, FAR), at_once(B0, NEAR)], 4: [at_once(A0, GROUP)]}
    by_h_phase(dgu0, WGU0, acc, 0, NF, (), late)
    rs(B0, FAR)
    by_h_end(acc, x, dh1, dx)
    rs(B0, GROUP)
    for u in range(len(UNITS)):
        wait(u, GROUP)


def finish(dx, *refs):
    parts, (dx_o, gate_o, up_o, down_o) = refs[:12], refs[12:]

    def body(dx_v, *vs):
        ins, (dx_w, *outs) = vs[:12], vs[12:]
        i = pl.program_id(0)
        dx_w[...] = dx_v[...]
        for layer, u in ((1, 0), (0, 3)):
            d, da, db = (ins[2 * (u + k) : 2 * (u + k) + 2] for k in range(3))
            gate_w, up_w, down_w = outs[3 * layer : 3 * layer + 3]
            down_w[...] = (d[0][...] + d[1][...].astype(F32)).astype(BF)
            for use, pair in ((i < 3, da), (i >= 3, db)):
                @pl.when(use)
                def _(pair=pair, gate_w=gate_w, up_w=up_w):
                    total = (pair[0][...] + pair[1][...].astype(F32)).astype(BF)
                    gate_w[...] = total[:, :FT]
                    up_w[...] = total[:, FT:]

    def cap(i):
        return jnp.minimum(i, 3)

    ins = [(dx, (512, D), lambda i: (cap(i), 0))]
    for u in range(6):
        shape = (RD_, D // 4) if u % 3 == 0 else (RU, W2)
        index = (
            (lambda i: (0, cap(i))),
            (lambda i: (0, jnp.minimum(i, 2))),
            (lambda i: (0, jnp.maximum(i - 3, 0))),
        )[u % 3]
        ins += [(parts[2 * u], shape, index), (parts[2 * u + 1], shape, index)]
    outs = [(dx_o.at[0], (512, D), lambda i: (cap(i), 0))]
    for layer in range(2):
        outs += [
            (gate_o.at[layer], (RU, FT), lambda i: (0, i)),
            (up_o.at[layer], (RU, FT), lambda i: (0, i)),
            (down_o.at[layer], (RD_, D // 4), lambda i: (0, cap(i))),
        ]
    run(body, (NF,), ins, outs)


def solution(mesh):
    def step(x, dy, w_gate, w_up, w_down):
        shapes = [((T, D), BF)]
        shapes += [((D, 2 * F), BF)] * 2 + [((F, D), BF)] * 2 + [((T, D), BF)] * 3
        shapes += [((T, F), BF)] + [((T, F), F32)] * 2 + [((T, 2 * F), BF)] * 2 + [((T, D), BF)]
        for unit in UNITS:
            shapes += unit_shapes(*unit)
        anywhere = pl.BlockSpec(memory_space=pl.ANY)

        def arrays(shapes):
            return [jax.ShapeDtypeStruct(s, t) for s, t in shapes]

        res = pl.pallas_call(
            kernel,
            out_shape=arrays(shapes),
            in_specs=[anywhere] * 5,
            out_specs=[anywhere] * len(shapes),
            scratch_shapes=[
                pltpu.VMEM((2, D, W2), BF),
                pltpu.VMEM((T, D), F32),
                pltpu.SemaphoreType.DMA((2,)),
                pltpu.SemaphoreType.DMA((NAG, 7)),
                pltpu.SemaphoreType.DMA((NAG, 7)),
                pltpu.SemaphoreType.DMA((6, 9)),
                pltpu.SemaphoreType.DMA((6, 9)),
            ],
            compiler_params=pltpu.CompilerParams(
                collective_id=0, has_side_effects=True, vmem_limit_bytes=62 * 2**20
            ),
            cost_estimate=pl.CostEstimate(flops=17 * 2 * T * D * F, bytes_accessed=2**30, transcendentals=0),
            name="step",
        )(x, dy, w_gate, w_up, w_down)
        last = [res[14 + 9 * u + k] for u in range(len(UNITS)) for k in (6, 8)]
        outs = [((1, T, D), BF), ((2, RU, F), BF), ((2, RU, F), BF), ((2, RD_, D), BF)]
        return pl.pallas_call(
            finish,
            out_shape=arrays(outs),
            in_specs=[anywhere] * 13,
            out_specs=[anywhere] * 4,
            compiler_params=pltpu.CompilerParams(vmem_limit_bytes=62 * 2**20),
            name="finish",
        )(res[0], *last)

    states, cut = P(("rep", "r", "s"), None, None), P(None, "s", None)
    return jax.shard_map(
        step,
        mesh=mesh,
        in_specs=(states, states) + (cut,) * 3,
        out_specs=(states,) + (P("rep", "s", None),) * 3,
        check_vma=False,
    )
```
